256 devices in a mesh: grp: 16 (over y, z_lo, core), seq: 16 (over x, z_hi).
Axes of the slice: x: 4, y: 4, z: 8 (z_hi: 4, z_lo: 2; z = z_hi * 2 + z_lo), core: 2. Of those that a mesh axis runs over, the one named last changes fastest.
Arguments:
- prefix_hidden: bfloat16 [16, 2048, 5120], P('grp', 'seq'), may hold values from -6 to 6
- prefix_keys: bfloat16 [16, 2048, 512], P('grp', 'seq'), may hold values from -6 to 6
- prefix_value_rows: bfloat16 [16, 2048, 512], P('grp', 'seq'), may hold values from -6 to 6
- comp_hidden: bfloat16 [16, 256, 5120], P('grp', 'seq'), may hold values from -6 to 6
- completion_queries: bfloat16 [16, 256, 2560], P('grp', 'seq'), may hold values from -6 to 6
- completion_keys: bfloat16 [16, 256, 512], P('grp', 'seq'), may hold values from -6 to 6
- completion_values: bfloat16 [16, 256, 512], P('grp', 'seq'), may hold values from -6 to 6
- out_grad: bfloat16 [16, 256, 2560], P('grp', 'seq'), may hold values from -6 to 6
- counts: int32 [16], P('grp'), may hold values from 4 to 16
- lengths: int32 [16, 16], P('grp', 'seq'), may hold values from 1 to 16
Outputs:
- attn_out: bfloat16 [16, 256, 2560], P('grp', 'seq')
- completion_query_gradient: bfloat16 [16, 256, 2560], P('grp', 'seq')
- comp_key_grad: bfloat16 [16, 256, 512], P('grp', 'seq')
- comp_value_grad: bfloat16 [16, 256, 512], P('grp', 'seq')
- prefix_key_grad: bfloat16 [16, 2048, 512], P('grp', 'seq')
- prefix_value_grad: bfloat16 [16, 2048, 512], P('grp', 'seq')
- value_proj_grad: float32 [5120, 512], P('seq')
The draws below stay inside these ranges and needn't reach their ends.
Inputs may be any that keep to these rules, and one draw needn't show every extreme that they name: Completion slots 0 to counts[g] - 1 of group g carry a completion; the others are empty. A completion occupies the first lengths[g, c] token slots of its slot.
All inputs are finite; a program needn't handle non-finite values.
Results may differ from the reference program's by a relative error of at most 0.013.
The reference program's roundings to bfloat16 on the way count: a program that leaves them out, or rounds other values in their place, can miss the bound.
Values may be sent and summed in bfloat16 or wider, within the bound.
No kernel may reach another device: no remote copies, remote signals or barrier semaphores. Data moves between devices by JAX's collectives and lax.ppermute only.
A program may use at most 64 MiB of HBM per device.

```python
import jax
import jax.numpy as jnp
from jax import lax

MODEL_WIDTH = 5120
HEAD_SIZE = 128
QUERY_HEADS = 20
KEY_VALUE_HEADS = 4
SLOT_LENGTH = 16
PREFIX_TOKENS = 2048
COMPLETION_SLOTS = 16
COMPLETION_TOKEN = 256
PROMPT_GROUPS = 16


def unsigned_entries(key, tag, dims_out):
    sub_key = jax.random.fold_in(key, tag)
    return jnp.clip(jax.random.normal(sub_key, dims_out, jnp.float32), -6.0, 6.0)


def draw_completion_queries(key, part):
    table_entries = unsigned_entries(key, 11, (PROMPT_GROUPS, COMPLETION_TOKEN, QUERY_HEADS * HEAD_SIZE))
    return table_entries.astype(jnp.bfloat16)


def draw_completion_keys(key, part):
    table_entries = unsigned_entries(key, 12, (PROMPT_GROUPS, COMPLETION_TOKEN, KEY_VALUE_HEADS * HEAD_SIZE))
    return table_entries.astype(jnp.bfloat16)


def draw_prefix_keys(key, part):
    table_entries = unsigned_entries(key, 13, (PROMPT_GROUPS, PREFIX_TOKENS, KEY_VALUE_HEADS * HEAD_SIZE))
    return table_entries.astype(jnp.bfloat16)


def place_ends(result, stream_key, least, largest):
    longest = result.shape.index(max(result.shape))
    spots = []
    for shift in (0, 1):
        where = [jax.random.randint(jax.random.fold_in(stream_key, axis), (), 0, length) for axis, length in enumerate(result.shape)]
        where[longest] = (where[longest] + shift) % result.shape[longest]
        spots.append(tuple(where))
    return result.at[spots[0]].set(least).at[spots[1]].set(largest)


def levels(key, dims, cuts, low, top_value):
    level, own = 1.0, jax.random.fold_in(key, 6)
    for axis_at, blocks in cuts:
        steps = jnp.exp(jax.random.uniform(jax.random.fold_in(own, axis_at), (blocks,), jnp.float32, low / len(cuts), top_value / len(cuts)))
        level = level * jnp.repeat(steps, dims[axis_at] // blocks).reshape([-1 if axis == axis_at else 1 for axis in range(len(dims))])
    return level


def scatter_about(key, shape, spread, limit, shards=(), kind=jnp.bfloat16):
    result = jax.random.normal(key, shape, jnp.float32) * spread
    if len(shards) > 0:
        result = levels(key, shape, shards, -0.22, 0.18) * result
    return jnp.clip(result, min=-limit, max=limit).astype(kind)


def setup_inputs(seed: int = 0) -> dict:
    keys = jax.random.split(jax.random.key(seed), 11)
    prefix_hidden = scatter_about(keys[0], (PROMPT_GROUPS, PREFIX_TOKENS, MODEL_WIDTH), 1.0, 6.0, ((0, 16), (1, 16)))
    prefix_keys = draw_prefix_keys(jax.random.fold_in(keys[10], 71), 0)
    prefix_value_rows = scatter_about(keys[2], (PROMPT_GROUPS, PREFIX_TOKENS, KEY_VALUE_HEADS * HEAD_SIZE), 1.0, 6.0, ((0, 16), (1, 16)))
    comp_hidden = scatter_about(keys[3], (PROMPT_GROUPS, COMPLETION_TOKEN, MODEL_WIDTH), 1.0, 6.0, ((0, 16), (1, 16)))
    completion_queries = draw_completion_queries(jax.random.fold_in(keys[10], 71), 0)
    completion_keys = draw_completion_keys(jax.random.fold_in(keys[10], 71), 0)
    completion_values = scatter_about(keys[6], (PROMPT_GROUPS, COMPLETION_TOKEN, KEY_VALUE_HEADS * HEAD_SIZE), 1.0, 6.0, ((0, 16), (1, 16)))
    out_grad = scatter_about(keys[7], (PROMPT_GROUPS, COMPLETION_TOKEN, QUERY_HEADS * HEAD_SIZE), 1.0, 6.0, ((0, 16), (1, 16)))
    counts = place_ends(jax.random.randint(keys[8], (PROMPT_GROUPS,), COMPLETION_SLOTS // 4, COMPLETION_SLOTS + 1), jax.random.fold_in(keys[8], 1), COMPLETION_SLOTS // 4, COMPLETION_SLOTS).astype(jnp.int32)
    lengths = place_ends(jax.random.randint(keys[9], (PROMPT_GROUPS, COMPLETION_SLOTS), 1, SLOT_LENGTH + 1), jax.random.fold_in(keys[9], 1), 1, SLOT_LENGTH).astype(jnp.int32)
    return {"prefix_hidden": prefix_hidden, "prefix_keys": prefix_keys, "prefix_value_rows": prefix_value_rows, "comp_hidden": comp_hidden, "completion_queries": completion_queries, "completion_keys": completion_keys, "completion_values": completion_values, "out_grad": out_grad, "counts": counts, "lengths": lengths}


NEG_BIG = -1.0e30


def round_trip(values):
    return lax.optimization_barrier(values.astype(jnp.bfloat16)).astype(jnp.float32)


def block_count(total):
    if total > 512 and total % 512 == 0:
        return total // 512
    return 1


def divided_blocks(rows):
    count = block_count(rows.shape[0])
    return rows.reshape((count, rows.shape[0] // count) + rows.shape[1:])


def to_rows(values):
    return jnp.transpose(values, (1, 2, 0, 3)).reshape(values.shape[1], values.shape[2], -1)


def from_rows(values, comps):
    return jnp.transpose(values.reshape(values.shape[0], values.shape[1], comps, -1), (2, 0, 1, 3))


def group_pass(hidden_pre, prefix_key_rows, prefix_value_part, hidden_comp, input_queries, input_keys, input_values, input_gradients, count, lens):
    head_repeat = QUERY_HEADS // KEY_VALUE_HEADS
    token_rows = COMPLETION_SLOTS * SLOT_LENGTH
    key_value_width = KEY_VALUE_HEADS * HEAD_SIZE
    scale = HEAD_SIZE ** -0.5
    query_rows = input_queries.astype(jnp.float32).reshape(token_rows, KEY_VALUE_HEADS, head_repeat, HEAD_SIZE)
    slot = jnp.arange(token_rows) // SLOT_LENGTH
    posit = jnp.arange(token_rows) % SLOT_LENGTH
    slot_len = jnp.sum(jnp.where(slot[:, None] == jnp.arange(COMPLETION_SLOTS)[None, :], lens[None, :], 0), axis=1)
    live_mask = ((slot < count) & (posit < slot_len)).astype(jnp.float32)
    output_gradient = (input_gradients.astype(jnp.float32) * live_mask[:, None]).reshape(token_rows, KEY_VALUE_HEADS, head_repeat, HEAD_SIZE)
    completion_query_rows = query_rows.reshape(COMPLETION_SLOTS, SLOT_LENGTH, KEY_VALUE_HEADS, head_repeat, HEAD_SIZE)
    completion_key_rows = input_keys.astype(jnp.float32).reshape(COMPLETION_SLOTS, SLOT_LENGTH, KEY_VALUE_HEADS, HEAD_SIZE)
    completion_value_rows = input_values.astype(jnp.float32).reshape(COMPLETION_SLOTS, SLOT_LENGTH, KEY_VALUE_HEADS, HEAD_SIZE)
    causal = jnp.arange(SLOT_LENGTH)[:, None] >= jnp.arange(SLOT_LENGTH)[None, :]
    own_scores = jnp.where(causal, jnp.einsum("ctkrd,cukd->ckrtu", completion_query_rows, completion_key_rows) * scale, NEG_BIG)
    own_max = jnp.max(own_scores, axis=-1)
    own_sum = jnp.sum(jnp.exp(own_scores - own_max[..., None]), axis=-1)
    key_block_list = divided_blocks(prefix_key_rows.astype(jnp.float32).reshape(PREFIX_TOKENS, KEY_VALUE_HEADS, HEAD_SIZE))
    value_block_list = divided_blocks(prefix_value_part.astype(jnp.float32).reshape(PREFIX_TOKENS, KEY_VALUE_HEADS, HEAD_SIZE))

    def scores_of(block):
        return jnp.einsum("tkrd,jkd->krtj", query_rows, block) * scale

    def add_stats(carry, block):
        high, total = carry
        scores = scores_of(block)
        new_high = jnp.maximum(high, jnp.max(scores, axis=-1))
        new_total = total * jnp.exp(high - new_high) + jnp.sum(jnp.exp(scores - new_high[..., None]), axis=-1)
        return (new_high, new_total), None

    stats, unused = lax.scan(add_stats, (to_rows(own_max), to_rows(own_sum)), key_block_list)
    lse = stats[0] + jnp.log(stats[1])
    own_probs = jnp.exp(own_scores - from_rows(lse, COMPLETION_SLOTS)[..., None])
    own_weights_narrow = round_trip(own_probs)
    context_rows = jnp.einsum("xsgav,xvsh->xasgh", own_weights_narrow, completion_value_rows).reshape(token_rows, KEY_VALUE_HEADS, head_repeat, HEAD_SIZE)

    def add_context(total, pair):
        probs = jnp.exp(scores_of(pair[0]) - lse[..., None])
        return total + jnp.einsum("krtj,jkd->tkrd", round_trip(probs), pair[1]), None

    context_rows, unused = lax.scan(add_context, context_rows, (key_block_list, value_block_list))
    attn = (context_rows * live_mask[:, None, None, None]).astype(jnp.bfloat16).reshape(token_rows, QUERY_HEADS * HEAD_SIZE)
    delta = jnp.transpose(jnp.sum(output_gradient * context_rows, axis=-1), (1, 2, 0))
    completion_output_gradient = output_gradient.reshape(COMPLETION_SLOTS, SLOT_LENGTH, KEY_VALUE_HEADS, head_repeat, HEAD_SIZE)
    own_dprob = jnp.einsum("ctkrd,cukd->ckrtu", completion_output_gradient, completion_value_rows)
    own_ds_b = round_trip(own_probs * (own_dprob - from_rows(delta, COMPLETION_SLOTS)[..., None]))
    own_query_gradient = jnp.einsum("xsgav,xvsh->xasgh", own_ds_b, completion_key_rows) * scale
    dk_own = jnp.einsum("ckrtu,ctkrd->cukd", own_ds_b, completion_query_rows) * scale
    dv_own = jnp.einsum("ckrtu,ctkrd->cukd", own_weights_narrow, completion_output_gradient)

    def prefix_gradient_list(total, pair):
        probs = jnp.exp(scores_of(pair[0]) - lse[..., None])
        probs_b = round_trip(probs)
        dprob = jnp.einsum("tkrd,jkd->krtj", output_gradient, pair[1])
        dscore_b = round_trip(probs * (dprob - delta[..., None]))
        total = total + jnp.einsum("krtj,jkd->tkrd", dscore_b, pair[0]) * scale
        key_part = jnp.einsum("krtj,tkrd->jkd", dscore_b, query_rows) * scale
        value_part = jnp.einsum("krtj,tkrd->jkd", probs_b, output_gradient)
        rows = pair[0].shape[0]
        return total, jnp.concatenate([key_part.reshape(rows, -1), value_part.reshape(rows, -1)], axis=1)

    prefix_query_gradient, gradient_blocks = lax.scan(prefix_gradient_list, jnp.zeros((token_rows, KEY_VALUE_HEADS, head_repeat, HEAD_SIZE), jnp.float32), (key_block_list, value_block_list))
    grad_terms = gradient_blocks.reshape(PREFIX_TOKENS, 2 * key_value_width)
    completion_query_gradient = (prefix_query_gradient + own_query_gradient.reshape(token_rows, KEY_VALUE_HEADS, head_repeat, HEAD_SIZE)).astype(jnp.bfloat16).reshape(token_rows, QUERY_HEADS * HEAD_SIZE)
    value_terms_comp = dv_own.reshape(token_rows, key_value_width)
    value_terms_pre = grad_terms[:, key_value_width:]
    comp_key_grad = dk_own.reshape(token_rows, key_value_width).astype(jnp.bfloat16)
    comp_value_grad = value_terms_comp.astype(jnp.bfloat16)
    prefix_key_grad = grad_terms[:, :key_value_width].astype(jnp.bfloat16)
    prefix_value_grad = value_terms_pre.astype(jnp.bfloat16)
    proj = jnp.dot(hidden_pre.astype(jnp.float32).T, value_terms_pre, precision=lax.Precision.HIGHEST)
    proj = proj + jnp.dot(hidden_comp.astype(jnp.float32).T, value_terms_comp, precision=lax.Precision.HIGHEST)
    return attn, completion_query_gradient, comp_key_grad, comp_value_grad, prefix_key_grad, prefix_value_grad, proj


def reference(prefix_hidden, prefix_keys, prefix_value_rows, comp_hidden, completion_queries, completion_keys, completion_values, out_grad, counts, lengths):
    def step(carry, items):
        results = group_pass(*items)
        return carry + results[6], results[:6]

    start_index = jnp.zeros((MODEL_WIDTH, KEY_VALUE_HEADS * HEAD_SIZE), jnp.float32)
    items = (prefix_hidden, prefix_keys, prefix_value_rows, comp_hidden, completion_queries, completion_keys, completion_values, out_grad, counts, lengths)
    total, stacked = lax.scan(step, start_index, items)
    return (stacked[0], stacked[1], stacked[2], stacked[3], stacked[4], stacked[5], total)
```

```python
import functools

import jax
import jax.numpy as jnp
from jax import lax
from jax.experimental import pallas as pl
from jax.experimental.pallas import tpu as pltpu
from jax.sharding import PartitionSpec as P

HEAD = 128
KV = 4
REP = 5
SLOT = 16
PRE = 128
QR = REP * SLOT
ROWS = 4 * QR
TOK = PRE + SLOT
WIDTH = 5120
NEG_BIG = -1e30
SCALE = HEAD**-0.5
F32 = jnp.float32
BF16 = jnp.bfloat16

O_Q, O_D, O_K, O_V, O_CK, O_CV, O_END = 0, 80, 160, 288, 416, 432, 448

X_GROUPS = [[4 * x + z for x in range(4)] for z in range(4)]
Z_GROUPS = [[4 * x + z for z in range(4)] for x in range(4)]

VM = pl.BlockSpec(memory_space=pltpu.VMEM)
SM = pl.BlockSpec(memory_space=pltpu.SMEM)


def mm(a, b, ca, cb):
    return lax.dot_general(a, b, (((ca,), (cb,)), ((), ())), preferred_element_type=F32)


def kernel_call(body, outs, ins, scratch=(), name=None):
    return pl.pallas_call(
        body,
        out_shape=outs,
        in_specs=ins,
        out_specs=jax.tree.map(lambda _: VM, outs),
        scratch_shapes=list(scratch),
        name=name,
        compiler_params=pltpu.CompilerParams(vmem_limit_bytes=48 * 1024 * 1024),
    )


def live_rows(info_ref):
    t = lax.broadcasted_iota(jnp.int32, (SLOT, 1), 0)
    return (info_ref[0] < info_ref[1]) & (t < info_ref[2])


def pack_body(info_ref, q_ref, d_ref, k_ref, v_ref, ck_ref, cv_ref, out_ref):
    live = live_rows(info_ref)
    for k in range(KV):
        for r in range(REP):
            cols = pl.ds((k * REP + r) * HEAD, HEAD)
            out_ref[k, O_Q + r * SLOT : O_Q + (r + 1) * SLOT] = q_ref[:, cols]
            dout = jnp.where(live, d_ref[:, cols].astype(F32), 0.0)
            out_ref[k, O_D + r * SLOT : O_D + (r + 1) * SLOT] = dout.astype(BF16)
        cols = pl.ds(k * HEAD, HEAD)
        out_ref[k, O_K:O_V] = k_ref[:, cols]
        out_ref[k, O_V:O_CK] = v_ref[:, cols]
        out_ref[k, O_CK:O_CV] = ck_ref[:, cols]
        out_ref[k, O_CV:O_END] = cv_ref[:, cols]


def own_mask():
    key = lax.broadcasted_iota(jnp.int32, (4 * SLOT, ROWS), 0)
    row = lax.broadcasted_iota(jnp.int32, (4 * SLOT, ROWS), 1)
    same = key // SLOT == row // QR
    return same & (key % SLOT <= row % SLOT)


def rows_of(ref, lo, hi):
    return ref[:, lo:hi].reshape(-1, HEAD)


def block_q(ref):
    return rows_of(ref, O_Q, O_D)


def block_d(ref):
    return rows_of(ref, O_D, O_K)


def own_scores(a_ref, q):
    raw = mm(rows_of(a_ref, O_CK, O_CV), q, 1, 1) * SCALE
    return jnp.where(own_mask(), raw, NEG_BIG)


def stats_body(info_ref, a_ref, b1_ref, b2_ref, b3_ref, out_ref):
    z = info_ref[3]
    keys = rows_of(a_ref, O_K, O_V)
    for s, ref in enumerate((a_ref, b1_ref, b2_ref, b3_ref)):
        q = block_q(ref)
        scores = mm(keys, q, 1, 1) * SCALE
        high = jnp.max(scores, axis=0, keepdims=True)
        if s == 0:
            own = own_scores(a_ref, q)
            high = jnp.maximum(high, jnp.max(own, axis=0, keepdims=True))
        total = jnp.sum(jnp.exp(scores - high), axis=0, keepdims=True)
        if s == 0:
            total = total + jnp.sum(jnp.exp(own - high), axis=0, keepdims=True)
        zb = lax.rem(z + 4 - s, 4)
        out_ref[pl.ds(zb, 1), :] = high
        out_ref[pl.ds(zb + 4, 1), :] = total


def joined_lse(stat_refs):
    highs = [r[0:4, :] for r in stat_refs]
    totals = [r[4:8, :] for r in stat_refs]
    high = functools.reduce(jnp.maximum, highs)
    total = sum(t * jnp.exp(h - high) for h, t in zip(highs, totals))
    return high + jnp.log(total)


def value_body(info_ref, a_ref, b1_ref, b2_ref, b3_ref, s0, s1, s2, s3, vt_ref, delta_ref, lse_ref):
    z = info_ref[3]
    keys = rows_of(a_ref, O_K, O_V)
    values = rows_of(a_ref, O_V, O_CK)
    lse_ref[...] = joined_lse((s0, s1, s2, s3))
    acc = jnp.zeros((4 * PRE, HEAD), F32)
    for s, ref in enumerate((a_ref, b1_ref, b2_ref, b3_ref)):
        q = block_q(ref)
        d = block_d(ref)
        zb = lax.rem(z + 4 - s, 4)
        lse = lse_ref[pl.ds(zb, 1), :]
        probs_b = jnp.exp(mm(keys, q, 1, 1) * SCALE - lse).astype(BF16)
        acc = acc + mm(probs_b, d, 1, 0)
        dprob = mm(values, d, 1, 1)
        delta = jnp.sum(probs_b.astype(F32) * dprob, axis=0, keepdims=True)
        if s == 0:
            own_b = jnp.exp(own_scores(a_ref, q) - lse).astype(BF16)
            own_acc = mm(own_b, d, 1, 0)
            own_dprob = mm(rows_of(a_ref, O_CV, O_END), d, 1, 1)
            delta = delta + jnp.sum(own_b.astype(F32) * own_dprob, axis=0, keepdims=True)
        delta_ref[pl.ds(zb, 1), :] = delta
    for x in range(4):
        vt_ref[x, 0:PRE] = acc[x * PRE : (x + 1) * PRE].astype(BF16)
        vt_ref[x, PRE:TOK] = own_acc[x * SLOT : (x + 1) * SLOT].astype(BF16)


def grad_body(
    info_ref, a_ref, b1_ref, b2_ref, b3_ref, lse_ref, d0, d1, d2, d3, ret_ref, dk_ref, delta_ref
):
    z = info_ref[3]
    keys = rows_of(a_ref, O_K, O_V)
    values = rows_of(a_ref, O_V, O_CK)
    delta_ref[...] = (d0[...] + d1[...]) + (d2[...] + d3[...])
    acc = jnp.zeros((4 * PRE, HEAD), F32)
    for s, ref in enumerate((a_ref, b1_ref, b2_ref, b3_ref)):
        q = block_q(ref)
        d = block_d(ref)
        zb = lax.rem(z + 4 - s, 4)
        lse = lse_ref[pl.ds(zb, 1), :]
        delta = delta_ref[pl.ds(zb, 1), :]
        probs = jnp.exp(mm(keys, q, 1, 1) * SCALE - lse)
        context = mm(probs.astype(BF16), values, 0, 0)
        ds = (probs * (mm(values, d, 1, 1) - delta)).astype(BF16)
        acc = acc + mm(ds, q, 1, 0)
        dq = mm(ds, keys, 0, 0)
        if s == 0:
            own_keys = rows_of(a_ref, O_CK, O_CV)
            own_values = rows_of(a_ref, O_CV, O_END)
            own = jnp.exp(own_scores(a_ref, q) - lse)
            context = context + mm(own.astype(BF16), own_values, 0, 0)
            own_ds = (own * (mm(own_values, d, 1, 1) - delta)).astype(BF16)
            own_acc = mm(own_ds, q, 1, 0)
            dq = dq + mm(own_ds, own_keys, 0, 0)
        dq = dq * SCALE
        for x in range(4):
            ret_ref[4 * x + zb, 0:QR] = context[x * QR : (x + 1) * QR].astype(BF16)
            ret_ref[4 * x + zb, QR : 2 * QR] = dq[x * QR : (x + 1) * QR].astype(BF16)
    for x in range(4):
        dk_ref[x, 0:PRE] = (acc[x * PRE : (x + 1) * PRE] * SCALE).astype(BF16)
        dk_ref[x, PRE:TOK] = (own_acc[x * SLOT : (x + 1) * SLOT] * SCALE).astype(BF16)


def project_body(h_ref, vt_ref, out_ref):
    hidden = h_ref[...].reshape(4 * TOK, WIDTH // 4)
    for h in range(KV):
        part = mm(hidden, vt_ref[h].reshape(4 * TOK, HEAD), 0, 0)
        for z in range(4):
            for b in range(4):
                lo = z * 320 + b * 80
                out_ref[4 * h + b, z] = part[lo : lo + 80].astype(BF16)


def sum_body(in_ref, out_ref):
    total = in_ref[0].astype(F32)
    for i in range(1, in_ref.shape[0]):
        total = total + in_ref[i].astype(F32)
    out_ref[...] = total.astype(out_ref.dtype)


def unpack_body(info_ref, ret_ref, dk_ref, vt_ref, at_ref, dq_ref, ck_ref, cv_ref, pk_ref, pv_ref):
    live = live_rows(info_ref)
    x = info_ref[4]
    for k in range(KV):
        for r in range(REP):
            cols = pl.ds((k * REP + r) * HEAD, HEAD)
            lo = r * SLOT
            ctx = sum(ret_ref[4 * k + p, lo : lo + SLOT].astype(F32) for p in range(4))
            at_ref[:, cols] = jnp.where(live, ctx, 0.0).astype(BF16)
            lo = QR + r * SLOT
            dq = sum(ret_ref[4 * k + p, lo : lo + SLOT].astype(F32) for p in range(4))
            dq_ref[:, cols] = dq.astype(BF16)
        cols = pl.ds(k * HEAD, HEAD)
        pk_ref[:, cols] = dk_ref[k, 0:PRE]
        ck_ref[:, cols] = dk_ref[k, PRE:TOK]
        pv_ref[:, cols] = vt_ref[k, x, 0:PRE]
        cv_ref[:, cols] = vt_ref[k, x, PRE:TOK]


def spread_body(in_ref, out_ref):
    for h in range(KV):
        for b in range(4):
            out_ref[b * 80 : (b + 1) * 80, h * HEAD : (h + 1) * HEAD] = in_ref[4 * h + b]


def sds(shape, dtype):
    return jax.ShapeDtypeStruct(shape, dtype)


def swap(array, groups):
    return lax.all_to_all(
        array, "seq", split_axis=0, concat_axis=0, tiled=True, axis_index_groups=groups
    )


def from_others(array, groups):
    out = []
    for s in (1, 2, 3):
        pairs = [(g[i], g[(i + s) % 4]) for g in groups for i in range(4)]
        out.append(lax.ppermute(array, "seq", pairs))
    return out


def per_device(
    prefix_hidden,
    prefix_keys,
    prefix_value_rows,
    comp_hidden,
    completion_queries,
    completion_keys,
    completion_values,
    out_grad,
    counts,
    lengths,
):
    place = lax.axis_index("seq")
    info = jnp.stack([place, counts[0], lengths[0, 0], place % 4, place // 4]).astype(jnp.int32)
    packed = kernel_call(pack_body, sds((4, O_END, HEAD), BF16), [SM] + [VM] * 6, name="pack")(
        info,
        completion_queries[0],
        out_grad[0],
        prefix_keys[0],
        prefix_value_rows[0],
        completion_keys[0],
        completion_values[0],
    )
    mine = swap(packed, X_GROUPS)
    others = from_others(mine[:, O_Q:O_K], Z_GROUPS)

    hidden = jnp.concatenate([prefix_hidden[0], comp_hidden[0]], axis=0)
    hidden = jnp.transpose(hidden.reshape(TOK, 4, WIDTH // 4), (1, 0, 2))
    hidden = swap(hidden, X_GROUPS)

    stats = kernel_call(stats_body, sds((8, ROWS), F32), [SM] + [VM] * 4, name="stats")(
        info, mine, *others
    )
    stats = [stats] + from_others(stats, Z_GROUPS)
    terms, delta, lse = kernel_call(
        value_body,
        (sds((4, TOK, HEAD), BF16), sds((4, ROWS), F32), sds((4, ROWS), F32)),
        [SM] + [VM] * 8,
        name="value",
    )(info, mine, *others, *stats)

    wide = jnp.broadcast_to(terms[None], (4,) + terms.shape)
    wide = swap(wide, X_GROUPS)
    part = kernel_call(project_body, sds((16, 4, 80, HEAD), BF16), [VM] * 2, name="project")(
        hidden, wide
    )
    part = lax.all_to_all(part, "grp", split_axis=0, concat_axis=0, tiled=True)
    part = kernel_call(sum_body, sds((4, 80, HEAD), BF16), [VM], name="sum_grp")(part)
    part = swap(part, Z_GROUPS)
    part = kernel_call(sum_body, sds((80, HEAD), F32), [VM], name="sum_z")(part)
    whole = jnp.broadcast_to(part[None], (16, 80, HEAD))
    whole = lax.all_to_all(whole, "grp", split_axis=0, concat_axis=0, tiled=True)
    value_proj_grad = kernel_call(spread_body, sds((320, 512), F32), [VM], name="spread")(whole)

    deltas = [delta] + from_others(delta, Z_GROUPS)
    back, dk = kernel_call(
        grad_body,
        (sds((16, 2 * QR, HEAD), BF16), sds((4, TOK, HEAD), BF16)),
        [SM] + [VM] * 9,
        scratch=[pltpu.VMEM((4, ROWS), F32)],
        name="grad",
    )(info, mine, *others, lse, *deltas)
    back = lax.all_to_all(back, "seq", split_axis=0, concat_axis=0, tiled=True)
    dk = swap(dk, X_GROUPS)
    attn, dq, ck, cv, pk, pv = kernel_call(
        unpack_body,
        (
            sds((SLOT, 2560), BF16),
            sds((SLOT, 2560), BF16),
            sds((SLOT, 512), BF16),
            sds((SLOT, 512), BF16),
            sds((PRE, 512), BF16),
            sds((PRE, 512), BF16),
        ),
        [SM] + [VM] * 3,
        name="unpack",
    )(info, back, dk, wide)
    return attn[None], dq[None], ck[None], cv[None], pk[None], pv[None], value_proj_grad


def solution(mesh):
    rows = P("grp", "seq", None)
    return jax.shard_map(
        per_device,
        mesh=mesh,
        in_specs=(rows,) * 8 + (P("grp"), P("grp", "seq")),
        out_specs=(rows,) * 6 + (P("seq", None),),
        check_vma=False,
    )
```
